32 devices in a mesh: dp: 4 (over z), seq: 2 (over x), tensor: 4 (over y, core).
Axes of the slice: x: 2, y: 2, z: 4, core: 2. Of those that a mesh axis runs over, the one named last changes fastest.
Arguments:
- hidden_in: bfloat16 [16384, 2880], P(('dp', 'seq', 'tensor')), parts along dimension 0, may hold values from -6 to 6
- norm_gain: float32 [2880], replicated, may hold values from 0.5 to 1.5
- conv_weight: float32 [4, 2880], replicated, may hold values from -3 to 3
- w_query: bfloat16 [2880, 2048], P(None, 'tensor'), may hold values from -32 to 32
- w_key: bfloat16 [2880, 512], P(None, 'tensor'), may hold values from -1 to 1
- w_value: bfloat16 [2880, 512], P(None, 'tensor'), may hold values from -0.109375 to 0.109375
- w_out: bfloat16 [2048, 2880], P('tensor'), may hold values from -0.125 to 0.125
- doc_ids: int32 [16384], P(('dp', 'seq')), parts along dimension 0, may hold values from 0 to 15, never falling along the last dimension, each value on 1 to 1024 neighbouring positions
Outputs:
- hidden_out: bfloat16 [16384, 2880], P(('dp', 'seq', 'tensor')), parts along dimension 0
The draws below stay inside these ranges and needn't reach their ends.
There are 4 independent parts, one for each index of `dp`. The reference program is written for one: setup_inputs(seed, part) draws one part's arguments, and reference() takes and returns one part's arrays. A program takes and returns all parts, laid end to end along the dimension named above; an argument that names none is the same for every part. Nothing has to cross between parts.
Inputs may be any that keep to these rules, and one draw needn't show every extreme that they name: `doc_ids`: document numbers never fall along a window's tokens.
All inputs are finite; a program needn't handle non-finite values.
Results may differ from the reference program's by a relative error of at most 0.011.
Values may be sent and summed in bfloat16 or wider, within the bound.
A program may use at most 128 MiB of HBM per device.

```python
import math
import jax
import jax.numpy as jnp
import numpy as np
from jax import lax

D = 2880
HEADS = 32
KV_HEADS = 8
HEAD = 64
KERNEL = 4
WINDOW = 128
QBLOCK = 512
TOKENS = 4096
DOC_MOST = 1024
DOCS = 16


def key_matrix(key):
    scale = 1.0 / math.sqrt(D)
    raw = jax.random.normal(jax.random.fold_in(key, 11), (D, KV_HEADS * HEAD), jnp.float32) * scale
    return jnp.clip(raw, -5.0 * scale, 5.0 * scale)


def draw_w_key(key, part):
    return key_matrix(key).astype(jnp.bfloat16)


def draw_w_query(key, part):
    noise = jax.random.normal(jax.random.fold_in(key, 13), (D, HEADS * HEAD), jnp.float32) * (1.0 / math.sqrt(D))
    return noise.astype(jnp.bfloat16)


def steps_of(rng, shape, pieces, least, high):
    level = 1.0
    for dim, blocks in pieces:
        draws = jax.random.uniform(jax.random.fold_in(jax.random.fold_in(rng, 6), dim), (blocks,), jnp.float32, least / len(pieces), high / len(pieces))
        level = level * jnp.repeat(jnp.exp(draws), shape[dim] // blocks).reshape((-1,) + (1,) * (len(shape) - 1 - dim))
    return level


def length_profile(number_of, total, reach, lean):
    loads = [(1 << 20) // math.isqrt(grade ** lean) + 1 for grade in range(2, number_of + 1)]
    surplus, given = total - reach - (number_of - 1), [1] * (number_of - 1)
    while surplus > 0:
        movable = [i for i in range(number_of - 1) if given[i] < reach]
        pool, left = sum([loads[i] for i in movable]), surplus
        for i in movable:
            addition = min(reach - given[i], max(1, left * loads[i] // pool), surplus)
            given[i] = given[i] + addition
            surplus = surplus - addition
    return np.array([reach] + given)


def uneven_parts(own_key, amount, total, reach, slope):
    if amount == 2:
        one = jax.random.randint(own_key, (), max(1, total - reach), min(reach, total - 1) + 1)
        return jnp.stack([one, total - one])
    lengths = jnp.asarray(length_profile(amount, total, reach, slope), jnp.int32)
    pairs = (amount - 1) // 2
    donor, sink = lengths[1:1 + 2 * pairs:2], lengths[2:2 + 2 * pairs:2]
    slack = jnp.minimum(donor - 1, reach - sink)
    moved = jax.random.randint(jax.random.fold_in(own_key, 1), (pairs,), 0, 1 << 20) % (slack + 1)
    lengths = lengths.at[1:1 + 2 * pairs:2].set(donor - moved).at[2:2 + 2 * pairs:2].set(sink + moved)
    return lengths[jax.random.permutation(jax.random.fold_in(own_key, 2), amount)]


def normal_values(stream_key, extent, deviation, most, split=(), kind=jnp.bfloat16):
    loudness = steps_of(stream_key, extent, split, -0.22, 0.18) if split else 1.0
    values = jax.random.normal(stream_key, extent, jnp.float32) * deviation * loudness
    return jnp.minimum(jnp.maximum(values, -most), most).astype(kind)


def setup_inputs(seed: int = 0, part: int = 0) -> dict:
    arg_keys = jax.random.split(jax.random.key(seed), 9)
    part_keys = jax.random.split(jax.random.fold_in(arg_keys[8], part), 9)
    return {
        "hidden_in": normal_values(part_keys[0], (TOKENS, D), 1.0, 6.0, ((0, 8),)),
        "norm_gain": jnp.clip(1.0 + 0.1 * jax.random.normal(arg_keys[1], (D,), jnp.float32), 0.5, 1.5),
        "conv_weight": normal_values(arg_keys[2], (KERNEL, D), 0.5, 3.0, (), jnp.float32),
        "w_query": draw_w_query(jax.random.fold_in(arg_keys[8], 71), part),
        "w_key": draw_w_key(jax.random.fold_in(arg_keys[8], 71), part),
        "w_value": normal_values(arg_keys[5], (D, KV_HEADS * HEAD), D ** -0.5, 0.109375, ((1, 4),)),
        "w_out": normal_values(arg_keys[6], (HEADS * HEAD, D), (HEADS * HEAD) ** -0.5, 0.125, ((0, 4),)),
        "doc_ids": jnp.searchsorted(jnp.cumsum(uneven_parts(part_keys[7], DOCS, TOKENS, DOC_MOST, 2)), jnp.arange(TOKENS), side="right").astype(jnp.int32),
    }


eps = 1e-05
rope_base = 150000.0

def rotate(values, positions):
    rows = values.shape[0]
    half = HEAD // 2
    frequency = jnp.exp(jnp.arange(half, dtype=jnp.float32) * (-2.0 * math.log(rope_base) / HEAD))
    angle = positions.astype(jnp.float32)[:, None] * frequency[None, :]
    cosine = jnp.cos(angle)[:, None, :]
    sine = jnp.sin(angle)[:, None, :]
    shaped = values.reshape(rows, -1, HEAD)
    first = shaped[:, :, :half]
    second = shaped[:, :, half:]
    turned = jnp.concatenate([first * cosine - second * sine, second * cosine + first * sine], axis=2)
    return turned.reshape(rows, -1)

def attend(queries, keys, values, query_pos, key_pos, query_doc, key_doc):
    scores = jnp.einsum('qhgd,khd->hgqk', queries.astype(jnp.float32), keys.astype(jnp.float32)) * (1.0 / math.sqrt(HEAD))
    visible = (key_pos[None, :] <= query_pos[:, None]) & (key_pos[None, :] > query_pos[:, None] - WINDOW)
    visible = visible & (key_pos[None, :] >= 0) & (key_doc[None, :] == query_doc[:, None])
    scores = jnp.where(visible[None, None, :, :], scores, -jnp.inf)
    largest = lax.optimization_barrier(jnp.max(scores, axis=3, keepdims=True))
    weights = jnp.exp(scores - largest)
    total = lax.optimization_barrier(jnp.sum(weights, axis=3))
    rounded = weights.astype(jnp.bfloat16)
    summed = jnp.einsum('hgqk,khd->qhgd', rounded.astype(jnp.float32), values.astype(jnp.float32))
    result = summed / jnp.transpose(total, (2, 0, 1))[:, :, :, None]
    return result.reshape(result.shape[0], -1).astype(jnp.bfloat16)

def reference(hidden_in, norm_gain, conv_weight, w_query, w_key, w_value, w_out, doc_ids):
    total_rows = hidden_in.shape[0]
    inputs = hidden_in.astype(jnp.float32)
    mean_square = lax.optimization_barrier(jnp.mean(inputs * inputs, axis=1, keepdims=True))
    normed = (inputs * lax.rsqrt(mean_square + eps) * norm_gain[None, :]).astype(jnp.bfloat16)
    padded = jnp.concatenate([jnp.zeros((KERNEL - 1, D), jnp.float32), normed.astype(jnp.float32)], axis=0)
    convolved = jnp.zeros((total_rows, D), jnp.float32)
    for tap in range(KERNEL):
        convolved = convolved + conv_weight[tap][None, :] * padded[KERNEL - 1 - tap:KERNEL - 1 - tap + total_rows]
    mixed = convolved.astype(jnp.bfloat16)
    positions = jnp.arange(total_rows, dtype=jnp.int32)
    queries = rotate(jnp.dot(mixed, w_query, preferred_element_type=jnp.float32), positions).astype(jnp.bfloat16)
    keys = rotate(jnp.dot(mixed, w_key, preferred_element_type=jnp.float32), positions).astype(jnp.bfloat16)
    values = jnp.dot(mixed, w_value, preferred_element_type=jnp.float32).astype(jnp.bfloat16)
    groups = HEADS // KV_HEADS
    query_four = queries.reshape(total_rows, KV_HEADS, groups, HEAD)
    key_pad = jnp.concatenate([jnp.zeros((WINDOW, KV_HEADS * HEAD), jnp.bfloat16), keys], axis=0).reshape(total_rows + WINDOW, KV_HEADS, HEAD)
    value_pad = jnp.concatenate([jnp.zeros((WINDOW, KV_HEADS * HEAD), jnp.bfloat16), values], axis=0).reshape(total_rows + WINDOW, KV_HEADS, HEAD)
    doc_pad = jnp.concatenate([jnp.full((WINDOW,), -1, jnp.int32), doc_ids.astype(jnp.int32)], axis=0)
    pos_pad = jnp.arange(total_rows + WINDOW, dtype=jnp.int32) - WINDOW

    def one_block(index):
        begin = (index * QBLOCK).astype(jnp.int32)
        block_q = lax.dynamic_slice_in_dim(query_four, begin, QBLOCK, 0)
        block_k = lax.dynamic_slice_in_dim(key_pad, begin, QBLOCK + WINDOW, 0)
        block_v = lax.dynamic_slice_in_dim(value_pad, begin, QBLOCK + WINDOW, 0)
        query_pos = lax.dynamic_slice_in_dim(positions, begin, QBLOCK, 0)
        key_pos = lax.dynamic_slice_in_dim(pos_pad, begin, QBLOCK + WINDOW, 0)
        query_doc = lax.dynamic_slice_in_dim(doc_ids.astype(jnp.int32), begin, QBLOCK, 0)
        key_doc = lax.dynamic_slice_in_dim(doc_pad, begin, QBLOCK + WINDOW, 0)
        return attend(block_q, block_k, block_v, query_pos, key_pos, query_doc, key_doc)
    blocks = lax.map(one_block, jnp.arange(total_rows // QBLOCK, dtype=jnp.int32))
    attended = blocks.reshape(total_rows, HEADS * HEAD)
    projected = jnp.dot(attended, w_out, preferred_element_type=jnp.float32)
    return (inputs + projected).astype(jnp.bfloat16)
```

```python
import math

import jax
import jax.numpy as jnp
from jax import lax
from jax.experimental import pallas as pl
from jax.experimental.pallas import tpu as pltpu
from jax.sharding import PartitionSpec as P

HEAD = 64
WINDOW = 128
HALO = 144
PAD = HALO - WINDOW
LANES = 128
eps = 1e-05
rope_base = 150000.0
BF = jnp.bfloat16
F32 = jnp.float32


def kernel(seq_size, tensor_size, hidden, gain, taps, wq, wk, wv, wout, doc_row, doc_col, cos, sin, out,
           ext, normed, mixed, wqkv, wo, q_s, k_s, v_s, att, acc, docs, bias,
           load_sem, y_s, y_r, x_s, x_r, z_s, z_r, n_s, n_r, d_s, d_r, h_s, h_r):
    rows, width = hidden.shape
    qc, kc = wq.shape[1], wk.shape[1]
    cols = qc + 2 * kc
    ntaps = taps.shape[0]
    full = rows + WINDOW
    dp, seq, tensor = lax.axis_index("dp"), lax.axis_index("seq"), lax.axis_index("tensor")

    def other(i, bit):
        return i + bit * (1 - 2 * ((i // bit) % 2))

    y_dev = (dp, seq, other(tensor, 2))
    n_dev = (dp, seq, other(tensor, 1))
    x_dev = (dp, other(seq, 1), tensor)
    z_dev = (other(dp, 1), seq, tensor)
    place = seq * tensor_size + tensor
    has_prev = place > 0
    has_next = place < seq_size * tensor_size - 1
    nxt, prv = place + 1, place - 1
    next_dev = (dp, nxt // tensor_size, nxt % tensor_size)
    prev_dev = (dp, prv // tensor_size, prv % tensor_size)
    MESH = pl.DeviceIdType.MESH

    barrier = pltpu.get_barrier_semaphore()
    for dev in (y_dev, n_dev, x_dev, z_dev):
        pl.semaphore_signal(barrier, inc=1, device_id=dev, device_id_type=MESH)

    @pl.when(has_prev)
    def _():
        pl.semaphore_signal(barrier, inc=1, device_id=prev_dev, device_id_type=MESH)

    @pl.when(has_next)
    def _():
        pl.semaphore_signal(barrier, inc=1, device_id=next_dev, device_id_type=MESH)

    load_w = [
        pltpu.make_async_copy(wq, wqkv.at[0, :, pl.ds(0, qc)], load_sem.at[0]),
        pltpu.make_async_copy(wk, wqkv.at[0, :, pl.ds(qc, kc)], load_sem.at[1]),
        pltpu.make_async_copy(wv, wqkv.at[0, :, pl.ds(qc + kc, kc)], load_sem.at[2]),
    ]
    load_o = pltpu.make_async_copy(wout, wo.at[0], load_sem.at[3])
    load_h = pltpu.make_async_copy(hidden, ext.at[pl.ds(HALO, rows)], load_sem.at[4])
    load_d = pltpu.make_async_copy(doc_row, docs.at[:, pl.ds(WINDOW, rows)], load_sem.at[5])
    for c in load_w:
        c.start()
    load_h.start()
    load_d.start()
    load_o.start()
    pl.semaphore_wait(barrier, 4 + jnp.where(has_prev, 1, 0) + jnp.where(has_next, 1, 0))

    halo_h = pltpu.make_async_remote_copy(
        src_ref=hidden.at[pl.ds(rows - HALO, HALO)], dst_ref=ext.at[pl.ds(0, HALO)],
        send_sem=h_s.at[0], recv_sem=h_r.at[0], device_id=next_dev, device_id_type=MESH)
    halo_d = pltpu.make_async_remote_copy(
        src_ref=doc_row.at[:, pl.ds(rows - WINDOW, WINDOW)], dst_ref=docs.at[:, pl.ds(0, WINDOW)],
        send_sem=h_s.at[1], recv_sem=h_r.at[1], device_id=next_dev, device_id_type=MESH)

    @pl.when(has_next)
    def _():
        halo_h.start()
        halo_d.start()

    wrow, orow = width // 4, qc // 4
    wpart = wrow // 3
    osize = (48, 48, 32) if orow == 128 else (orow // 2, orow // 4, orow // 4)
    ostart = (0, osize[0], osize[0] + osize[1])

    def part(buf, slot, q, j):
        if buf == 0:
            return wqkv.at[slot, pl.ds(pl.multiple_of(q * wrow + j * wpart, 16), wpart)]
        return wo.at[slot, pl.ds(pl.multiple_of(q * orow + ostart[j], 16), osize[j])]

    xb, zb = seq % 2, dp % 2
    quarter = (xb * 2 + zb, (1 - xb) * 2 + zb, xb * 2 + 1 - zb, (1 - xb) * 2 + 1 - zb)
    sent = []

    def copy(buf, role, j, src_slot, dst_slot, ss, rs, k, dev):
        return pltpu.make_async_remote_copy(
            src_ref=part(buf, src_slot, quarter[role], j), dst_ref=part(buf, dst_slot, quarter[role], j),
            send_sem=ss.at[buf, k], recv_sem=rs.at[buf, k], device_id=dev, device_id_type=MESH)

    def go(c):
        c.start()
        sent.append(c)

    def y_copy(buf, k):
        role, j = ((0, 0), (0, 1), (0, 2), (3, 2))[k]
        return copy(buf, role, j, 0, 2, y_s, y_r, k, y_dev)

    def x_send(buf, k):
        role, j = ((0, 0), (0, 1), (0, 2), (2, 1))[k]
        return copy(buf, role, j, 2, 2, x_s, x_r, k, x_dev)

    def x_recv(buf, k):
        role, j = ((1, 0), (1, 1), (1, 2), (3, 1))[k]
        return copy(buf, role, j, 2, 2, x_s, x_r, k, x_dev)

    def z_send(buf, k):
        role, j = ((0, 0), (0, 1), (0, 2), (1, 0))[k]
        return copy(buf, role, j, 2, 2, z_s, z_r, k, z_dev)

    def z_recv(buf, k):
        role, j = ((2, 0), (2, 1), (2, 2), (3, 0))[k]
        return copy(buf, role, j, 2, 2, z_s, z_r, k, z_dev)

    def n_copy(buf, role, j):
        return copy(buf, role, j, 2, 3, n_s, n_r, role * 3 + j, n_dev)

    def direct(buf):
        whole = (wqkv, wo)[buf]
        return pltpu.make_async_remote_copy(
            src_ref=whole.at[0], dst_ref=whole.at[1], send_sem=d_s.at[buf], recv_sem=d_r.at[buf],
            device_id=n_dev, device_id_type=MESH)

    def from_y(buf, k):
        y_wait = y_recv(buf, k)
        y_wait.wait_recv()
        if k < 3:
            go(x_send(buf, k))
            go(z_send(buf, k))
            go(n_copy(buf, 0, k))
        else:
            go(n_copy(buf, 3, 2))

    def y_recv(buf, k):
        return y_copy(buf, k)

    def from_x(buf, k):
        x_recv(buf, k).wait_recv()
        if k == 0:
            go(z_send(buf, 3))
        if k < 3:
            go(n_copy(buf, 1, k))
        else:
            go(n_copy(buf, 3, 1))

    def from_z(buf, k):
        z_recv(buf, k).wait_recv()
        if k == 1:
            go(x_send(buf, 3))
        if k < 3:
            go(n_copy(buf, 2, k))
        else:
            go(n_copy(buf, 3, 0))

    for c in load_w:
        c.wait()
    for k in range(4):
        go(y_copy(0, k))
    go(direct(0))
    load_h.wait()
    load_d.wait()
    load_o.wait()
    for k in range(4):
        go(y_copy(1, k))
    go(direct(1))

    def norm_rows(lo, hi):
        @pl.loop(lo // 16, hi // 16)
        def _(i):
            r = pl.ds(pl.multiple_of(i * 16, 16), 16)
            h = ext[r, :].astype(F32)
            ms = jnp.mean(h * h, axis=1, keepdims=True)
            normed[r, :] = (h * lax.rsqrt(ms + eps) * gain[...]).astype(BF).astype(F32)

    def conv_rows(lo, hi):
        @pl.loop(lo // 16, hi // 16)
        def _(i):
            block = normed[pl.ds(pl.multiple_of(i * 16 + PAD - 8, 8), 24), :]
            total = jnp.zeros((16, width), F32)
            for k in range(ntaps):
                total = total + taps[k : k + 1, :] * block[8 - k : 24 - k]
            mixed[pl.ds(pl.multiple_of(i * 16, 16), 16), :] = total.astype(BF)

    norm_rows(HALO, HALO + rows)
    conv_rows(WINDOW + 16, full)
    from_y(0, 0)

    @pl.when(has_prev)
    def _():
        halo_h.wait_recv()
        halo_d.wait_recv()

    @pl.when(jnp.logical_not(has_prev))
    def _():
        ext[0:HALO, :] = jnp.zeros((HALO, width), BF)
        docs[:, 0:WINDOW] = jnp.full((docs.shape[0], WINDOW), -1, jnp.int32)

    norm_rows(0, HALO)
    conv_rows(0, WINDOW + 16)

    blocks = rows // WINDOW
    span = 2 * WINDOW
    rel_r = lax.broadcasted_iota(jnp.int32, (WINDOW, span), 0)
    rel_c = lax.broadcasted_iota(jnp.int32, (WINDOW, span), 1)
    in_window = (rel_c > rel_r) & (rel_c <= rel_r + WINDOW)
    for i in range(blocks):
        qd = doc_col[i * WINDOW : (i + 1) * WINDOW, :]
        kd = docs[0:1, i * WINDOW : i * WINDOW + span]
        same = jnp.concatenate([qd, qd], axis=1) == kd
        bias[i] = jnp.where(in_window & same, 0.0, -jnp.inf)

    def turn(x, c, s):
        lane = lax.broadcasted_iota(jnp.int32, x.shape, 1)
        swapped = jnp.where(lane % HEAD < HEAD // 2, pltpu.roll(x, LANES - HEAD // 2, 1), pltpu.roll(x, HEAD // 2, 1))
        return x * c + swapped * s

    scale = 1.0 / math.sqrt(HEAD)

    def project(slot):
        @pl.loop(0, qc // 256)
        def _(n):
            c0 = pl.multiple_of(n * 256, 256)
            r = jnp.dot(mixed[WINDOW:, :], wqkv[slot, :, pl.ds(c0, 256)], preferred_element_type=F32)
            for h in range(2):
                piece = r[:, h * LANES : (h + 1) * LANES]
                q_s[n * 2 + h] = (turn(piece, cos[WINDOW:, :], sin[WINDOW:, :]) * scale).astype(BF)

        r = jnp.dot(mixed[...], wqkv[slot, :, qc:], preferred_element_type=F32)
        k = turn(r[:, :kc], cos[...], sin[...])
        v = r[:, kc:]
        low = lax.broadcasted_iota(jnp.int32, k.shape, 1) < HEAD
        kr, vr = pltpu.roll(k, HEAD, 1), pltpu.roll(v, HEAD, 1)
        k_s[0] = jnp.where(low, k, kr).astype(BF)
        k_s[1] = jnp.where(low, kr, k).astype(BF)
        ones = jnp.ones((full, LANES), BF)
        v_s[0, :, :LANES] = jnp.where(low, v, vr).astype(BF)
        v_s[1, :, :LANES] = jnp.where(low, vr, v).astype(BF)
        v_s[0, :, LANES:] = ones
        v_s[1, :, LANES:] = ones

    def attend(slot):
        @pl.loop(0, blocks)
        def _(i):
            r0 = pl.multiple_of(i * WINDOW, WINDOW)
            low = lax.broadcasted_iota(jnp.int32, (WINDOW, LANES), 1) < HEAD
            zero = jnp.zeros((WINDOW, LANES), BF)
            for g in range(2):
                stack = []
                for h in range(2):
                    qv = q_s[g * 2 + h, pl.ds(r0, WINDOW), :]
                    stack += [jnp.where(low, qv, zero), jnp.where(low, zero, qv)]
                qs = jnp.concatenate(stack, axis=0)
                ks = k_s[g, pl.ds(r0, span), :]
                s = lax.dot_general(qs, ks, (((1,), (1,)), ((), ())), preferred_element_type=F32)
                s = s.reshape(4, WINDOW, span) + bias[i][None]
                m = jnp.max(s, axis=2, keepdims=True)
                p = jnp.exp(s - m).astype(BF).reshape(4 * WINDOW, span)
                o = jnp.dot(p, v_s[g, pl.ds(r0, span), :], preferred_element_type=F32)
                o = o[:, :LANES] / o[:, LANES:]
                for h in range(2):
                    a = o[(2 * h) * WINDOW : (2 * h + 1) * WINDOW]
                    b = o[(2 * h + 1) * WINDOW : (2 * h + 2) * WINDOW]
                    c0 = (g * 2 + h) * LANES
                    att[slot % 2, pl.ds(r0, WINDOW), c0 : c0 + LANES] = jnp.where(low, a, b).astype(BF)

    def out_cols(first, c, n, last):
        two = None
        for s in range(2):
            r = jnp.dot(att[s], wo[first + s, :, pl.ds(c, n)], preferred_element_type=F32)
            two = r if two is None else two + r
        if last:
            two = two + acc[:, pl.ds(c, n)]
            out[:, pl.ds(c, n)] = (ext[HALO:, pl.ds(c, n)].astype(F32) + two).astype(BF)
        else:
            acc[:, pl.ds(c, n)] = two

    def project_out(first, last, lo, hi):
        @pl.loop(lo, hi)
        def _(n):
            out_cols(first, pl.multiple_of(n * 256, 256), 256, last)

    whole = width // 256
    rest = width - whole * 256

    project(0)
    from_y(0, 1)
    attend(0)
    from_x(0, 0)
    from_z(0, 0)
    direct(0).wait_recv()
    project(1)
    from_y(0, 2)
    from_x(0, 1)
    from_z(0, 1)
    attend(1)
    direct(1).wait_recv()
    project_out(0, False, 0, whole // 2)
    from_y(0, 3)
    from_x(0, 2)
    from_z(0, 2)
    project_out(0, False, whole // 2, whole)
    if rest:
        out_cols(0, whole * 256, rest, False)
    from_x(0, 3)
    from_z(0, 3)
    from_y(1, 0)
    project(2)
    from_y(1, 1)
    from_x(1, 0)
    from_z(1, 0)
    attend(2)
    for role in range(4):
        for j in range(3):
            n_copy(0, role, j).wait_recv()
    from_y(1, 2)
    from_x(1, 1)
    from_z(1, 1)
    project(3)
    from_y(1, 3)
    from_x(1, 2)
    from_z(1, 2)
    attend(3)
    from_x(1, 3)
    from_z(1, 3)
    for role in range(4):
        for j in range(3):
            n_copy(1, role, j).wait_recv()
    project_out(2, True, 0, whole)
    if rest:
        out_cols(2, whole * 256, rest, True)
    for c in sent:
        c.wait_send()

    @pl.when(has_next)
    def _():
        halo_h.wait_send()
        halo_d.wait_send()


def solution(mesh):
    seq_size, tensor_size = mesh.shape["seq"], mesh.shape["tensor"]

    def local(hidden_in, norm_gain, conv_weight, w_query, w_key, w_value, w_out, doc_ids):
        rows, width = hidden_in.shape
        qc, kc = w_query.shape[1], w_key.shape[1]
        full = rows + WINDOW
        tensor = lax.axis_index("tensor")
        begin = (lax.axis_index("seq") * tensor_size + tensor) * rows
        mine = lax.dynamic_slice_in_dim(doc_ids, tensor * rows, rows, 0)
        doc_row = jnp.broadcast_to(mine[None, :], (8, rows))
        doc_col = jnp.broadcast_to(mine[:, None], (rows, LANES))
        half = HEAD // 2
        frequency = jnp.exp(jnp.arange(half, dtype=F32) * (-2.0 * math.log(rope_base) / HEAD))
        positions = (begin - WINDOW + jnp.arange(full, dtype=jnp.int32)).astype(F32)
        angle = positions[:, None] * frequency[None, :]
        c, s = jnp.cos(angle), jnp.sin(angle)
        cos = jnp.concatenate([c, c, c, c], axis=1)
        sin = jnp.concatenate([-s, s, -s, s], axis=1)
        dma = pltpu.SemaphoreType.DMA
        vm, hb = pl.BlockSpec(memory_space=pltpu.VMEM), pl.BlockSpec(memory_space=pl.ANY)
        return pl.pallas_call(
            lambda *refs: kernel(seq_size, tensor_size, *refs),
            out_shape=jax.ShapeDtypeStruct((rows, width), BF),
            in_specs=[hb, vm, vm, hb, hb, hb, hb, hb, vm, vm, vm],
            out_specs=vm,
            scratch_shapes=[
                pltpu.VMEM((HALO + rows, width), BF),
                pltpu.VMEM((HALO + rows, width), F32),
                pltpu.VMEM((full, width), BF),
                pltpu.VMEM((4, width, qc + 2 * kc), BF),
                pltpu.VMEM((4, qc, width), BF),
                pltpu.VMEM((qc // LANES, rows, LANES), BF),
                pltpu.VMEM((2, full, LANES), BF),
                pltpu.VMEM((2, full, 2 * LANES), BF),
                pltpu.VMEM((2, rows, qc), BF),
                pltpu.VMEM((rows, width), F32),
                pltpu.VMEM((8, full), jnp.int32),
                pltpu.VMEM((rows // WINDOW, WINDOW, 2 * WINDOW), F32),
                dma((6,)),
                dma((2, 4)), dma((2, 4)),
                dma((2, 4)), dma((2, 4)),
                dma((2, 4)), dma((2, 4)),
                dma((2, 12)), dma((2, 12)),
                dma((2,)), dma((2,)),
                dma((2,)), dma((2,)),
            ],
            compiler_params=pltpu.CompilerParams(
                collective_id=0, has_side_effects=True, vmem_limit_bytes=67043328),
            name="block",
        )(hidden_in, norm_gain[None, :], conv_weight, w_query, w_key, w_value, w_out, doc_row, doc_col, cos, sin)

    in_specs = (
        P(("dp", "seq", "tensor"), None),
        P(),
        P(),
        P(None, "tensor"),
        P(None, "tensor"),
        P(None, "tensor"),
        P("tensor", None),
        P(("dp", "seq")),
    )
    out_specs = P(("dp", "seq", "tensor"), None)
    return jax.shard_map(local, mesh=mesh, in_specs=in_specs, out_specs=out_specs, check_vma=False)
```

```python
import math

import jax
import jax.numpy as jnp
from jax import lax
from jax.experimental import pallas as pl
from jax.experimental.pallas import tpu as pltpu
from jax.sharding import PartitionSpec as P

HEAD = 64
WINDOW = 128
HALO = 144
PAD = HALO - WINDOW
LANES = 128
eps = 1e-05
rope_base = 150000.0
BF = jnp.bfloat16
F32 = jnp.float32


def kernel(seq_size, tensor_size, hidden, gain, taps, wq, wk, wv, wout, halo, doc_row, cos, sin, out,
           own, ext, normed, mixed, wqkv, wo, q_s, k_s, v_s, att, acc, docs, bias,
           load_sem, y_s, y_r, x_s, x_r, z_s, z_r, n_s, n_r, d_s, d_r, h_s, h_r):
    width, rows = hidden.shape
    qc, kc = wq.shape[1], wk.shape[1]
    cols = qc + 2 * kc
    ntaps = taps.shape[0]
    full = rows + WINDOW
    dp, seq, tensor = lax.axis_index("dp"), lax.axis_index("seq"), lax.axis_index("tensor")

    def other(i, bit):
        return i + bit * (1 - 2 * ((i // bit) % 2))

    y_dev = (dp, seq, other(tensor, 2))
    n_dev = (dp, seq, other(tensor, 1))
    x_dev = (dp, other(seq, 1), tensor)
    z_dev = (other(dp, 1), seq, tensor)
    place = seq * tensor_size + tensor
    has_prev = place > 0
    has_next = place < seq_size * tensor_size - 1
    nxt, prv = place + 1, place - 1
    next_dev = (dp, nxt // tensor_size, nxt % tensor_size)
    prev_dev = (dp, prv // tensor_size, prv % tensor_size)
    MESH = pl.DeviceIdType.MESH

    barrier = pltpu.get_barrier_semaphore()
    for dev in (y_dev, n_dev, x_dev, z_dev):
        pl.semaphore_signal(barrier, inc=1, device_id=dev, device_id_type=MESH)

    @pl.when(has_prev)
    def _():
        pl.semaphore_signal(barrier, inc=1, device_id=prev_dev, device_id_type=MESH)

    @pl.when(has_next)
    def _():
        pl.semaphore_signal(barrier, inc=1, device_id=next_dev, device_id_type=MESH)

    load_w = [
        pltpu.make_async_copy(wq, wqkv.at[0, :, pl.ds(0, qc)], load_sem.at[0]),
        pltpu.make_async_copy(wk, wqkv.at[0, :, pl.ds(qc, kc)], load_sem.at[1]),
        pltpu.make_async_copy(wv, wqkv.at[0, :, pl.ds(qc + kc, kc)], load_sem.at[2]),
    ]
    load_o = pltpu.make_async_copy(wout, wo.at[0], load_sem.at[3])
    load_h = pltpu.make_async_copy(hidden, own, load_sem.at[4])
    load_d = pltpu.make_async_copy(doc_row, docs.at[:, pl.ds(WINDOW, rows)], load_sem.at[5])
    for c in load_w:
        c.start()
    load_h.start()
    load_d.start()
    load_o.start()
    pl.semaphore_wait(barrier, 4 + jnp.where(has_prev, 1, 0) + jnp.where(has_next, 1, 0))

    halo_h = pltpu.make_async_remote_copy(
        src_ref=halo, dst_ref=ext.at[pl.ds(0, HALO)],
        send_sem=h_s.at[0], recv_sem=h_r.at[0], device_id=next_dev, device_id_type=MESH)
    halo_d = pltpu.make_async_remote_copy(
        src_ref=doc_row.at[:, pl.ds(rows - WINDOW, WINDOW)], dst_ref=docs.at[:, pl.ds(0, WINDOW)],
        send_sem=h_s.at[1], recv_sem=h_r.at[1], device_id=next_dev, device_id_type=MESH)

    @pl.when(has_next)
    def _():
        halo_h.start()
        halo_d.start()

    wrow = width // 4
    wpart = wrow // 3

    def part(buf, slot, q, j):
        return (wqkv, wo)[buf].at[slot, pl.ds(pl.multiple_of(q * wrow + j * wpart, 16), wpart)]

    xb, zb = seq % 2, dp % 2
    quarter = (xb * 2 + zb, (1 - xb) * 2 + zb, xb * 2 + 1 - zb, (1 - xb) * 2 + 1 - zb)
    sent = []

    def copy(buf, role, j, src_slot, dst_slot, ss, rs, k, dev):
        return pltpu.make_async_remote_copy(
            src_ref=part(buf, src_slot, quarter[role], j), dst_ref=part(buf, dst_slot, quarter[role], j),
            send_sem=ss.at[buf, k], recv_sem=rs.at[buf, k], device_id=dev, device_id_type=MESH)

    def go(c):
        c.start()
        sent.append(c)

    def y_copy(buf, k):
        role, j = ((0, 0), (0, 1), (0, 2), (3, 2))[k]
        return copy(buf, role, j, 0, 2, y_s, y_r, k, y_dev)

    def x_send(buf, k):
        role, j = ((0, 0), (0, 1), (0, 2), (2, 1))[k]
        return copy(buf, role, j, 2, 2, x_s, x_r, k, x_dev)

    def x_recv(buf, k):
        role, j = ((1, 0), (1, 1), (1, 2), (3, 1))[k]
        return copy(buf, role, j, 2, 2, x_s, x_r, k, x_dev)

    def z_send(buf, k):
        role, j = ((0, 0), (0, 1), (0, 2), (1, 0))[k]
        return copy(buf, role, j, 2, 2, z_s, z_r, k, z_dev)

    def z_recv(buf, k):
        role, j = ((2, 0), (2, 1), (2, 2), (3, 0))[k]
        return copy(buf, role, j, 2, 2, z_s, z_r, k, z_dev)

    def n_copy(buf, role, j):
        return copy(buf, role, j, 2, 3, n_s, n_r, role * 3 + j, n_dev)

    def direct(buf):
        whole = (wqkv, wo)[buf]
        return pltpu.make_async_remote_copy(
            src_ref=whole.at[0], dst_ref=whole.at[1], send_sem=d_s.at[buf], recv_sem=d_r.at[buf],
            device_id=n_dev, device_id_type=MESH)

    def from_y(buf, k):
        y_wait = y_recv(buf, k)
        y_wait.wait_recv()
        if k < 3:
            go(x_send(buf, k))
            go(z_send(buf, k))
            go(n_copy(buf, 0, k))
        else:
            go(n_copy(buf, 3, 2))

    def y_recv(buf, k):
        return y_copy(buf, k)

    def from_x(buf, k):
        x_recv(buf, k).wait_recv()
        if k == 0:
            go(z_send(buf, 3))
        if k < 3:
            go(n_copy(buf, 1, k))
        else:
            go(n_copy(buf, 3, 1))

    def from_z(buf, k):
        z_recv(buf, k).wait_recv()
        if k == 1:
            go(x_send(buf, 3))
        if k < 3:
            go(n_copy(buf, 2, k))
        else:
            go(n_copy(buf, 3, 0))

    for c in load_w:
        c.wait()
    for k in range(4):
        go(y_copy(0, k))
    go(direct(0))
    load_h.wait()
    load_d.wait()
    load_o.wait()
    for k in range(4):
        go(y_copy(1, k))
    go(direct(1))

    def norm_rows(lo, hi):
        @pl.loop(lo // 16, hi // 16)
        def _(i):
            r = pl.ds(pl.multiple_of(i * 16, 16), 16)
            h = ext[r, :].astype(F32)
            ms = jnp.mean(h * h, axis=1, keepdims=True)
            normed[r, :] = (h * lax.rsqrt(ms + eps) * gain[...]).astype(BF).astype(F32)

    def conv_rows(lo, hi):
        @pl.loop(lo // 16, hi // 16)
        def _(i):
            block = normed[pl.ds(pl.multiple_of(i * 16 + PAD - 8, 8), 24), :]
            total = jnp.zeros((16, width), F32)
            for k in range(ntaps):
                total = total + taps[k : k + 1, :] * block[8 - k : 24 - k]
            mixed[pl.ds(pl.multiple_of(i * 16, 16), 16), :] = total.astype(BF)

    def flip(c, n):
        ext[HALO:, pl.ds(c, n)] = own[pl.ds(c, n), :].astype(F32).T.astype(BF)

    @pl.loop(0, width // LANES)
    def _(i):
        flip(pl.multiple_of(i * LANES, LANES), LANES)

    if width % LANES:
        flip(width // LANES * LANES, width % LANES)
    norm_rows(HALO, HALO + rows)
    conv_rows(WINDOW + 16, full)
    from_y(0, 0)

    @pl.when(has_prev)
    def _():
        halo_h.wait_recv()
        halo_d.wait_recv()

    @pl.when(jnp.logical_not(has_prev))
    def _():
        ext[0:HALO, :] = jnp.zeros((HALO, width), BF)
        docs[:, 0:WINDOW] = jnp.full((docs.shape[0], WINDOW), -1, jnp.int32)

    norm_rows(0, HALO)
    conv_rows(0, WINDOW + 16)

    blocks = rows // WINDOW
    span = 2 * WINDOW
    rel_r = lax.broadcasted_iota(jnp.int32, (WINDOW, span), 0)
    rel_c = lax.broadcasted_iota(jnp.int32, (WINDOW, span), 1)
    in_window = (rel_c > rel_r) & (rel_c <= rel_r + WINDOW)
    for i in range(blocks):
        qd = docs[0:1, (i + 1) * WINDOW : (i + 2) * WINDOW].astype(F32)
        qd = jnp.broadcast_to(qd, (WINDOW, WINDOW)).T
        kd = docs[0:1, i * WINDOW : i * WINDOW + span].astype(F32)
        same = jnp.concatenate([qd, qd], axis=1) == kd
        bias[i] = jnp.where(in_window & same, 0.0, -jnp.inf)

    def turn(x, c, s):
        lane = lax.broadcasted_iota(jnp.int32, x.shape, 1)
        swapped = jnp.where(lane % HEAD < HEAD // 2, pltpu.roll(x, LANES - HEAD // 2, 1), pltpu.roll(x, HEAD // 2, 1))
        return x * c + swapped * s

    scale = 1.0 / math.sqrt(HEAD)

    def project(slot):
        @pl.loop(0, qc // 256)
        def _(n):
            c0 = pl.multiple_of(n * 256, 256)
            r = jnp.dot(mixed[WINDOW:, :], wqkv[slot, :, pl.ds(c0, 256)], preferred_element_type=F32)
            for h in range(2):
                piece = r[:, h * LANES : (h + 1) * LANES]
                q_s[n * 2 + h] = (turn(piece, cos[WINDOW:, :], sin[WINDOW:, :]) * scale).astype(BF)

        r = jnp.dot(mixed[...], wqkv[slot, :, qc:], preferred_element_type=F32)
        k = turn(r[:, :kc], cos[...], sin[...])
        v = r[:, kc:]
        low = lax.broadcasted_iota(jnp.int32, k.shape, 1) < HEAD
        kr, vr = pltpu.roll(k, HEAD, 1), pltpu.roll(v, HEAD, 1)
        k_s[0] = jnp.where(low, k, kr).astype(BF)
        k_s[1] = jnp.where(low, kr, k).astype(BF)
        ones = jnp.ones((full, LANES), BF)
        v_s[0, :, :LANES] = jnp.where(low, v, vr).astype(BF)
        v_s[1, :, :LANES] = jnp.where(low, vr, v).astype(BF)
        v_s[0, :, LANES:] = ones
        v_s[1, :, LANES:] = ones

    def attend(slot):
        @pl.loop(0, blocks)
        def _(i):
            r0 = pl.multiple_of(i * WINDOW, WINDOW)
            low = lax.broadcasted_iota(jnp.int32, (WINDOW, LANES), 1) < HEAD
            zero = jnp.zeros((WINDOW, LANES), BF)
            for g in range(2):
                stack = []
                for h in range(2):
                    qv = q_s[g * 2 + h, pl.ds(r0, WINDOW), :]
                    stack += [jnp.where(low, qv, zero), jnp.where(low, zero, qv)]
                qs = jnp.concatenate(stack, axis=0)
                ks = k_s[g, pl.ds(r0, span), :]
                s = lax.dot_general(qs, ks, (((1,), (1,)), ((), ())), preferred_element_type=F32)
                s = s.reshape(4, WINDOW, span) + bias[i][None]
                m = jnp.max(s, axis=2, keepdims=True)
                p = jnp.exp(s - m).astype(BF).reshape(4 * WINDOW, span)
                o = jnp.dot(p, v_s[g, pl.ds(r0, span), :], preferred_element_type=F32)
                o = o[:, :LANES] / o[:, LANES:]
                for h in range(2):
                    a = o[(2 * h) * WINDOW : (2 * h + 1) * WINDOW]
                    b = o[(2 * h + 1) * WINDOW : (2 * h + 2) * WINDOW]
                    c0 = (g * 2 + h) * LANES
                    att[slot % 2, c0 : c0 + LANES, pl.ds(r0, WINDOW)] = jnp.where(low, a, b).T.astype(BF)

    step = width // 6

    def project_out(first, last, lo, hi):
        @pl.loop(lo, hi)
        def _(n):
            r = pl.ds(pl.multiple_of(n * step, 16), step)
            two = jnp.dot(wo[first, r, :], att[0], preferred_element_type=F32)
            two = two + jnp.dot(wo[first + 1, r, :], att[1], preferred_element_type=F32)
            if last:
                out[r, :] = (own[r, :].astype(F32) + (two + acc[r, :])).astype(BF)
            else:
                acc[r, :] = two

    project(0)
    from_y(0, 1)
    attend(0)
    from_x(0, 0)
    from_z(0, 0)
    direct(0).wait_recv()
    project(1)
    from_y(0, 2)
    from_x(0, 1)
    from_z(0, 1)
    attend(1)
    direct(1).wait_recv()
    project_out(0, False, 0, 3)
    from_y(0, 3)
    from_x(0, 2)
    from_z(0, 2)
    project_out(0, False, 3, 6)
    from_x(0, 3)
    from_z(0, 3)
    from_y(1, 0)
    project(2)
    from_y(1, 1)
    from_x(1, 0)
    from_z(1, 0)
    attend(2)
    for role in range(4):
        for j in range(3):
            n_copy(0, role, j).wait_recv()
    from_y(1, 2)
    from_x(1, 1)
    from_z(1, 1)
    project(3)
    from_y(1, 3)
    from_x(1, 2)
    from_z(1, 2)
    attend(3)
    from_x(1, 3)
    from_z(1, 3)
    for role in range(4):
        for j in range(3):
            n_copy(1, role, j).wait_recv()
    project_out(2, True, 0, 6)
    for c in sent:
        c.wait_send()

    @pl.when(has_next)
    def _():
        halo_h.wait_send()
        halo_d.wait_send()


def solution(mesh):
    seq_size, tensor_size = mesh.shape["seq"], mesh.shape["tensor"]

    def local(hidden_in, norm_gain, conv_weight, w_query, w_key, w_value, w_out, doc_ids):
        rows, width = hidden_in.shape
        qc, kc = w_query.shape[1], w_key.shape[1]
        full = rows + WINDOW
        tensor = lax.axis_index("tensor")
        begin = (lax.axis_index("seq") * tensor_size + tensor) * rows
        mine = lax.dynamic_slice_in_dim(doc_ids, tensor * rows, rows, 0)
        doc_row = jnp.broadcast_to(mine[None, :], (8, rows))
        half = HEAD // 2
        lane = jnp.arange(LANES, dtype=jnp.int32)
        frequency = jnp.exp((lane % half).astype(F32) * (-2.0 * math.log(rope_base) / HEAD))
        positions = (begin - WINDOW + jnp.arange(full, dtype=jnp.int32)).astype(F32)
        angle = positions[:, None] * frequency[None, :]
        cos = jnp.cos(angle)
        sin = jnp.sin(angle) * jnp.where(lane % HEAD < half, -1.0, 1.0)[None, :]
        dma = pltpu.SemaphoreType.DMA
        vm, hb = pl.BlockSpec(memory_space=pltpu.VMEM), pl.BlockSpec(memory_space=pl.ANY)
        return pl.pallas_call(
            lambda *refs: kernel(seq_size, tensor_size, *refs),
            out_shape=jax.ShapeDtypeStruct((width, rows), BF),
            in_specs=[hb, vm, vm, hb, hb, hb, hb, hb, hb, vm, vm],
            out_specs=vm,
            scratch_shapes=[
                pltpu.VMEM((width, rows), BF),
                pltpu.VMEM((HALO + rows, width), BF),
                pltpu.VMEM((HALO + rows, width), F32),
                pltpu.VMEM((full, width), BF),
                pltpu.VMEM((4, width, qc + 2 * kc), BF),
                pltpu.VMEM((4, width, qc), BF),
                pltpu.VMEM((qc // LANES, rows, LANES), BF),
                pltpu.VMEM((2, full, LANES), BF),
                pltpu.VMEM((2, full, 2 * LANES), BF),
                pltpu.VMEM((2, qc, rows), BF),
                pltpu.VMEM((width, rows), F32),
                pltpu.VMEM((8, full), jnp.int32),
                pltpu.VMEM((rows // WINDOW, WINDOW, 2 * WINDOW), F32),
                dma((6,)),
                dma((2, 4)), dma((2, 4)),
                dma((2, 4)), dma((2, 4)),
                dma((2, 4)), dma((2, 4)),
                dma((2, 12)), dma((2, 12)),
                dma((2,)), dma((2,)),
                dma((2,)), dma((2,)),
            ],
            compiler_params=pltpu.CompilerParams(
                collective_id=0, has_side_effects=True, vmem_limit_bytes=67043328),
            name="block",
        )(hidden_in.T, norm_gain[None, :], conv_weight, w_query, w_key, w_value, w_out.T,
          hidden_in[rows - HALO :], doc_row, cos, sin).T

    in_specs = (
        P(("dp", "seq", "tensor"), None),
        P(),
        P(),
        P(None, "tensor"),
        P(None, "tensor"),
        P(None, "tensor"),
        P("tensor", None),
        P(("dp", "seq")),
    )
    out_specs = P(("dp", "seq", "tensor"), None)
    return jax.shard_map(local, mesh=mesh, in_specs=in_specs, out_specs=out_specs, check_vma=False)
```

```python
import math

import jax
import jax.numpy as jnp
from jax import lax
from jax.experimental import pallas as pl
from jax.experimental.pallas import tpu as pltpu
from jax.sharding import PartitionSpec as P

HEAD = 64
WINDOW = 128
HALO = 144
PAD = HALO - WINDOW
LANES = 128
eps = 1e-05
rope_base = 150000.0
BF = jnp.bfloat16
F32 = jnp.float32


def kernel(seq_size, tensor_size, hidden, gain, taps, wq, wk, wv, wout, halo, doc_row, cos, sin, out,
           own, ext, normed, mixed, wqkv, wo, q_s, k_s, v_s, att, acc, docs, bias,
           load_sem, y_s, y_r, x_s, x_r, z_s, z_r, n_s, n_r, d_s, d_r, h_s, h_r):
    width, rows = hidden.shape
    qc, kc = wq.shape[1], wk.shape[1]
    cols = qc + 2 * kc
    ntaps = taps.shape[0]
    full = rows + WINDOW
    dp, seq, tensor = lax.axis_index("dp"), lax.axis_index("seq"), lax.axis_index("tensor")

    def other(i, bit):
        return i + bit * (1 - 2 * ((i // bit) % 2))

    y_dev = (dp, seq, other(tensor, 2))
    n_dev = (dp, seq, other(tensor, 1))
    x_dev = (dp, other(seq, 1), tensor)
    z_dev = (other(dp, 1), seq, tensor)
    place = seq * tensor_size + tensor
    has_prev = place > 0
    has_next = place < seq_size * tensor_size - 1
    nxt, prv = place + 1, place - 1
    next_dev = (dp, nxt // tensor_size, nxt % tensor_size)
    prev_dev = (dp, prv // tensor_size, prv % tensor_size)
    MESH = pl.DeviceIdType.MESH

    barrier = pltpu.get_barrier_semaphore()
    for dev in (y_dev, n_dev, x_dev, z_dev):
        pl.semaphore_signal(barrier, inc=1, device_id=dev, device_id_type=MESH)

    @pl.when(has_prev)
    def _():
        pl.semaphore_signal(barrier, inc=1, device_id=prev_dev, device_id_type=MESH)

    @pl.when(has_next)
    def _():
        pl.semaphore_signal(barrier, inc=1, device_id=next_dev, device_id_type=MESH)

    load_w = [
        pltpu.make_async_copy(wq, wqkv.at[0, :, pl.ds(0, qc)], load_sem.at[0]),
        pltpu.make_async_copy(wk, wqkv.at[0, :, pl.ds(qc, kc)], load_sem.at[1]),
        pltpu.make_async_copy(wv, wqkv.at[0, :, pl.ds(qc + kc, kc)], load_sem.at[2]),
    ]
    load_o = pltpu.make_async_copy(wout, wo.at[0], load_sem.at[3])
    load_h = pltpu.make_async_copy(hidden, own, load_sem.at[4])
    load_d = pltpu.make_async_copy(doc_row, docs.at[:, pl.ds(WINDOW, rows)], load_sem.at[5])
    for c in load_w:
        c.start()
    load_h.start()
    load_d.start()
    load_o.start()
    pl.semaphore_wait(barrier, 4 + jnp.where(has_prev, 1, 0) + jnp.where(has_next, 1, 0))

    halo_h = pltpu.make_async_remote_copy(
        src_ref=halo, dst_ref=ext.at[pl.ds(0, HALO)],
        send_sem=h_s.at[0], recv_sem=h_r.at[0], device_id=next_dev, device_id_type=MESH)
    halo_d = pltpu.make_async_remote_copy(
        src_ref=doc_row.at[:, pl.ds(rows - WINDOW, WINDOW)], dst_ref=docs.at[:, pl.ds(0, WINDOW)],
        send_sem=h_s.at[1], recv_sem=h_r.at[1], device_id=next_dev, device_id_type=MESH)

    wrow = width // 4
    wpart = wrow // 3

    def part(buf, slot, q, j):
        return (wqkv, wo)[buf].at[slot, pl.ds(pl.multiple_of(q * wrow + j * wpart, 16), wpart)]

    xb, zb = seq % 2, dp % 2
    quarter = (xb * 2 + zb, (1 - xb) * 2 + zb, xb * 2 + 1 - zb, (1 - xb) * 2 + 1 - zb)
    sent = []

    def copy(buf, role, j, src_slot, dst_slot, ss, rs, k, dev):
        return pltpu.make_async_remote_copy(
            src_ref=part(buf, src_slot, quarter[role], j), dst_ref=part(buf, dst_slot, quarter[role], j),
            send_sem=ss.at[buf, k], recv_sem=rs.at[buf, k], device_id=dev, device_id_type=MESH)

    def go(c):
        c.start()
        sent.append(c)

    def y_copy(buf, k):
        role, j = ((0, 0), (0, 1), (0, 2), (3, 2))[k]
        return copy(buf, role, j, 0, 2, y_s, y_r, k, y_dev)

    def x_send(buf, k):
        role, j = ((0, 0), (0, 1), (0, 2), (2, 1))[k]
        return copy(buf, role, j, 2, 2, x_s, x_r, k, x_dev)

    def x_recv(buf, k):
        role, j = ((1, 0), (1, 1), (1, 2), (3, 1))[k]
        return copy(buf, role, j, 2, 2, x_s, x_r, k, x_dev)

    def z_send(buf, k):
        role, j = ((0, 0), (0, 1), (0, 2), (1, 0))[k]
        return copy(buf, role, j, 2, 2, z_s, z_r, k, z_dev)

    def z_recv(buf, k):
        role, j = ((2, 0), (2, 1), (2, 2), (3, 0))[k]
        return copy(buf, role, j, 2, 2, z_s, z_r, k, z_dev)

    def n_copy(buf, role, j):
        return copy(buf, role, j, 2, 3, n_s, n_r, role * 3 + j, n_dev)

    def direct(buf):
        whole = (wqkv, wo)[buf]
        return pltpu.make_async_remote_copy(
            src_ref=whole.at[0], dst_ref=whole.at[1], send_sem=d_s.at[buf], recv_sem=d_r.at[buf],
            device_id=n_dev, device_id_type=MESH)

    def from_y(buf, k):
        y_wait = y_recv(buf, k)
        y_wait.wait_recv()
        if k < 3:
            go(x_send(buf, k))
            go(z_send(buf, k))
            go(n_copy(buf, 0, k))
        else:
            go(n_copy(buf, 3, 2))

    def y_recv(buf, k):
        return y_copy(buf, k)

    def from_x(buf, k):
        x_recv(buf, k).wait_recv()
        if k == 0:
            go(z_send(buf, 3))
        if k < 3:
            go(n_copy(buf, 1, k))
        else:
            go(n_copy(buf, 3, 1))

    def from_z(buf, k):
        z_recv(buf, k).wait_recv()
        if k == 1:
            go(x_send(buf, 3))
        if k < 3:
            go(n_copy(buf, 2, k))
        else:
            go(n_copy(buf, 3, 0))

    for c in load_w:
        c.wait()
    go(y_copy(0, 0))

    @pl.when(has_next)
    def _():
        halo_h.start()
        halo_d.start()

    for k in range(1, 4):
        go(y_copy(0, k))
    go(direct(0))
    load_h.wait()
    load_d.wait()
    load_o.wait()
    for k in range(4):
        go(y_copy(1, k))
    go(direct(1))

    def norm_rows(lo, hi):
        @pl.loop(lo // 16, hi // 16)
        def _(i):
            r = pl.ds(pl.multiple_of(i * 16, 16), 16)
            h = ext[r, :].astype(F32)
            ms = jnp.mean(h * h, axis=1, keepdims=True)
            normed[r, :] = (h * lax.rsqrt(ms + eps) * gain[...]).astype(BF).astype(F32)

    def conv_rows(lo, hi):
        @pl.loop(lo // 16, hi // 16)
        def _(i):
            block = normed[pl.ds(pl.multiple_of(i * 16 + PAD - 8, 8), 24), :]
            total = jnp.zeros((16, width), F32)
            for k in range(ntaps):
                total = total + taps[k : k + 1, :] * block[8 - k : 24 - k]
            mixed[pl.ds(pl.multiple_of(i * 16, 16), 16), :] = total.astype(BF)

    def flip(c, n):
        ext[HALO:, pl.ds(c, n)] = own[pl.ds(c, n), :].astype(F32).T.astype(BF)

    @pl.loop(0, width // LANES)
    def _(i):
        flip(pl.multiple_of(i * LANES, LANES), LANES)

    if width % LANES:
        flip(width // LANES * LANES, width % LANES)
    norm_rows(HALO, HALO + rows)
    conv_rows(WINDOW + 16, full)
    from_y(0, 0)

    @pl.when(has_prev)
    def _():
        halo_h.wait_recv()
        halo_d.wait_recv()

    @pl.when(jnp.logical_not(has_prev))
    def _():
        ext[0:HALO, :] = jnp.zeros((HALO, width), BF)
        docs[:, 0:WINDOW] = jnp.full((docs.shape[0], WINDOW), -1, jnp.int32)

    norm_rows(0, HALO)
    conv_rows(0, WINDOW + 16)

    blocks = rows // WINDOW
    span = 2 * WINDOW
    rel_r = lax.broadcasted_iota(jnp.int32, (WINDOW, span), 0)
    rel_c = lax.broadcasted_iota(jnp.int32, (WINDOW, span), 1)
    in_window = (rel_c > rel_r) & (rel_c <= rel_r + WINDOW)
    for i in range(blocks):
        qd = docs[0:1, (i + 1) * WINDOW : (i + 2) * WINDOW].astype(F32)
        qd = jnp.broadcast_to(qd, (WINDOW, WINDOW)).T
        kd = docs[0:1, i * WINDOW : i * WINDOW + span].astype(F32)
        same = jnp.concatenate([qd, qd], axis=1) == kd
        bias[i] = jnp.where(in_window & same, 0.0, -jnp.inf)

    def turn(x, c, s):
        lane = lax.broadcasted_iota(jnp.int32, x.shape, 1)
        swapped = jnp.where(lane % HEAD < HEAD // 2, pltpu.roll(x, LANES - HEAD // 2, 1), pltpu.roll(x, HEAD // 2, 1))
        return x * c + swapped * s

    scale = 1.0 / math.sqrt(HEAD)

    def project(slot):
        @pl.loop(0, qc // 256)
        def _(n):
            c0 = pl.multiple_of(n * 256, 256)
            r = jnp.dot(mixed[WINDOW:, :], wqkv[slot, :, pl.ds(c0, 256)], preferred_element_type=F32)
            for h in range(2):
                piece = r[:, h * LANES : (h + 1) * LANES]
                q_s[n * 2 + h] = (turn(piece, cos[WINDOW:, :], sin[WINDOW:, :]) * scale).astype(BF)

        r = jnp.dot(mixed[...], wqkv[slot, :, qc:], preferred_element_type=F32)
        k = turn(r[:, :kc], cos[...], sin[...])
        v = r[:, kc:]
        low = lax.broadcasted_iota(jnp.int32, k.shape, 1) < HEAD
        kr, vr = pltpu.roll(k, HEAD, 1), pltpu.roll(v, HEAD, 1)
        k_s[0] = jnp.where(low, k, kr).astype(BF)
        k_s[1] = jnp.where(low, kr, k).astype(BF)
        ones = jnp.ones((full, LANES), BF)
        v_s[0, :, :LANES] = jnp.where(low, v, vr).astype(BF)
        v_s[1, :, :LANES] = jnp.where(low, vr, v).astype(BF)
        v_s[0, :, LANES:] = ones
        v_s[1, :, LANES:] = ones

    def attend(slot):
        @pl.loop(0, blocks)
        def _(i):
            r0 = pl.multiple_of(i * WINDOW, WINDOW)
            low = lax.broadcasted_iota(jnp.int32, (WINDOW, LANES), 1) < HEAD
            zero = jnp.zeros((WINDOW, LANES), BF)
            for g in range(2):
                stack = []
                for h in range(2):
                    qv = q_s[g * 2 + h, pl.ds(r0, WINDOW), :]
                    stack += [jnp.where(low, qv, zero), jnp.where(low, zero, qv)]
                qs = jnp.concatenate(stack, axis=0)
                ks = k_s[g, pl.ds(r0, span), :]
                s = lax.dot_general(qs, ks, (((1,), (1,)), ((), ())), preferred_element_type=F32)
                s = s.reshape(4, WINDOW, span) + bias[i][None]
                m = jnp.max(s, axis=2, keepdims=True)
                p = jnp.exp(s - m).astype(BF).reshape(4 * WINDOW, span)
                o = jnp.dot(p, v_s[g, pl.ds(r0, span), :], preferred_element_type=F32)
                o = o[:, :LANES] / o[:, LANES:]
                for h in range(2):
                    a = o[(2 * h) * WINDOW : (2 * h + 1) * WINDOW]
                    b = o[(2 * h + 1) * WINDOW : (2 * h + 2) * WINDOW]
                    c0 = (g * 2 + h) * LANES
                    att[slot % 2, c0 : c0 + LANES, pl.ds(r0, WINDOW)] = jnp.where(low, a, b).T.astype(BF)

    step = width // 6

    def project_out(first, last, lo, hi):
        @pl.loop(lo, hi)
        def _(n):
            r = pl.ds(pl.multiple_of(n * step, 16), step)
            two = jnp.dot(wo[first, r, :], att[0], preferred_element_type=F32)
            two = two + jnp.dot(wo[first + 1, r, :], att[1], preferred_element_type=F32)
            if last:
                out[r, :] = (own[r, :].astype(F32) + (two + acc[r, :])).astype(BF)
            else:
                acc[r, :] = two

    project(0)
    from_y(0, 1)
    attend(0)
    from_x(0, 0)
    from_z(0, 0)
    direct(0).wait_recv()
    project(1)
    from_y(0, 2)
    from_x(0, 1)
    from_z(0, 1)
    attend(1)
    direct(1).wait_recv()
    project_out(0, False, 0, 3)
    from_y(0, 3)
    from_x(0, 2)
    from_z(0, 2)
    project_out(0, False, 3, 6)
    from_x(0, 3)
    from_z(0, 3)
    from_y(1, 0)
    project(2)
    from_y(1, 1)
    from_x(1, 0)
    from_z(1, 0)
    attend(2)
    for role in range(4):
        for j in range(3):
            n_copy(0, role, j).wait_recv()
    from_y(1, 2)
    from_x(1, 1)
    from_z(1, 1)
    project(3)
    from_y(1, 3)
    from_x(1, 2)
    from_z(1, 2)
    attend(3)
    from_x(1, 3)
    from_z(1, 3)
    for role in range(4):
        for j in range(3):
            n_copy(1, role, j).wait_recv()
    project_out(2, True, 0, 6)
    for c in sent:
        c.wait_send()

    @pl.when(has_next)
    def _():
        halo_h.wait_send()
        halo_d.wait_send()


def solution(mesh):
    seq_size, tensor_size = mesh.shape["seq"], mesh.shape["tensor"]

    def local(hidden_in, norm_gain, conv_weight, w_query, w_key, w_value, w_out, doc_ids):
        rows, width = hidden_in.shape
        qc, kc = w_query.shape[1], w_key.shape[1]
        full = rows + WINDOW
        tensor = lax.axis_index("tensor")
        begin = (lax.axis_index("seq") * tensor_size + tensor) * rows
        mine = lax.dynamic_slice_in_dim(doc_ids, tensor * rows, rows, 0)
        doc_row = jnp.broadcast_to(mine[None, :], (8, rows))
        half = HEAD // 2
        lane = jnp.arange(LANES, dtype=jnp.int32)
        frequency = jnp.exp((lane % half).astype(F32) * (-2.0 * math.log(rope_base) / HEAD))
        positions = (begin - WINDOW + jnp.arange(full, dtype=jnp.int32)).astype(F32)
        angle = positions[:, None] * frequency[None, :]
        cos = jnp.cos(angle)
        sin = jnp.sin(angle) * jnp.where(lane % HEAD < half, -1.0, 1.0)[None, :]
        dma = pltpu.SemaphoreType.DMA
        vm, hb = pl.BlockSpec(memory_space=pltpu.VMEM), pl.BlockSpec(memory_space=pl.ANY)
        return pl.pallas_call(
            lambda *refs: kernel(seq_size, tensor_size, *refs),
            out_shape=jax.ShapeDtypeStruct((width, rows), BF),
            in_specs=[hb, vm, vm, hb, hb, hb, hb, hb, hb, vm, vm],
            out_specs=vm,
            scratch_shapes=[
                pltpu.VMEM((width, rows), BF),
                pltpu.VMEM((HALO + rows, width), BF),
                pltpu.VMEM((HALO + rows, width), F32),
                pltpu.VMEM((full, width), BF),
                pltpu.VMEM((4, width, qc + 2 * kc), BF),
                pltpu.VMEM((4, width, qc), BF),
                pltpu.VMEM((qc // LANES, rows, LANES), BF),
                pltpu.VMEM((2, full, LANES), BF),
                pltpu.VMEM((2, full, 2 * LANES), BF),
                pltpu.VMEM((2, qc, rows), BF),
                pltpu.VMEM((width, rows), F32),
                pltpu.VMEM((8, full), jnp.int32),
                pltpu.VMEM((rows // WINDOW, WINDOW, 2 * WINDOW), F32),
                dma((6,)),
                dma((2, 4)), dma((2, 4)),
                dma((2, 4)), dma((2, 4)),
                dma((2, 4)), dma((2, 4)),
                dma((2, 12)), dma((2, 12)),
                dma((2,)), dma((2,)),
                dma((2,)), dma((2,)),
            ],
            compiler_params=pltpu.CompilerParams(
                collective_id=0, has_side_effects=True, vmem_limit_bytes=67043328),
            name="block",
        )(hidden_in.T, norm_gain[None, :], conv_weight, w_query, w_key, w_value, w_out.T,
          hidden_in[rows - HALO :], doc_row, cos, sin).T

    in_specs = (
        P(("dp", "seq", "tensor"), None),
        P(),
        P(),
        P(None, "tensor"),
        P(None, "tensor"),
        P(None, "tensor"),
        P("tensor", None),
        P(("dp", "seq")),
    )
    out_specs = P(("dp", "seq", "tensor"), None)
    return jax.shard_map(local, mesh=mesh, in_specs=in_specs, out_specs=out_specs, check_vma=False)
```
